32 devices in a mesh: dp: 1 (over z), ep: 32 (over y, x, core).
Axes of the slice: x: 4, y: 4, z: 1, core: 2. Of those that a mesh axis runs over, the one named last changes fastest.
The devices are a block of a 4x4x8 slice.
Arguments:
- tokens: bfloat16 [131072, 1024], P(('dp', 'ep'))
- choice_idx: int32 [32, 8192], P(('dp', 'ep'))
- gate_weight: float32 [32, 8192], P(('dp', 'ep'))
- w_in: bfloat16 [32, 1024, 4096], P('ep')
- w_out: bfloat16 [32, 4096, 1024], P('ep')
Outputs:
- output: bfloat16 [131072, 1024], P(('dp', 'ep'))
All inputs are finite; a program needn't handle non-finite values.
Results may differ from the reference program's by a relative error of at most 0.00637701.
Values are sent between devices in bfloat16 or wider.
A program may use at most 768 MiB of HBM per device.

```python
import jax
import jax.numpy as jnp
from jax import lax

D_MODEL = 1024
D_FF = 4096
EXPERTS = 32
TOKENS = 131072
CAPACITY = 8192
GROUP_SIZE = 32


def draw_routing(route_key):
    tok_local = TOKENS // GROUP_SIZE
    slots_dev = (EXPERTS // GROUP_SIZE) * CAPACITY
    base_share = slots_dev // GROUP_SIZE
    hot_rows = tok_local // 8
    cold_rows = tok_local - hot_rows
    half_group = GROUP_SIZE // 2
    route_keys = jax.random.split(route_key, 6)
    dev_grid = jnp.tile(jnp.arange(GROUP_SIZE, dtype=jnp.int32)[None, :], (GROUP_SIZE, 1))
    src_perm = jax.random.permutation(route_keys[0], dev_grid, axis=1, independent=True)
    pair_delta = jax.random.randint(route_keys[1], (GROUP_SIZE, half_group), 0, base_share + 1)
    pair_delta = pair_delta.at[:, 0].set(base_share)
    perm_counts = jnp.stack([base_share + pair_delta, base_share - pair_delta], axis=2).reshape(GROUP_SIZE, GROUP_SIZE)
    dest_ids = jnp.arange(GROUP_SIZE)[:, None]
    counts = jnp.zeros((GROUP_SIZE, GROUP_SIZE), jnp.int32).at[dest_ids, src_perm].set(perm_counts)
    block_ends = jnp.cumsum(counts, axis=1)
    starts = block_ends - counts
    slot_pos = jnp.arange(slots_dev, dtype=jnp.int32)
    src_of = jax.vmap(lambda end_row: jnp.searchsorted(end_row, slot_pos, side="right"))(block_ends)
    within = slot_pos[None, :] - jnp.take_along_axis(starts, src_of, axis=1)
    block_len = jnp.take_along_axis(counts, src_of, axis=1)
    hot_count = jnp.minimum(block_len // 2, hot_rows)
    hot_off = jax.random.randint(route_keys[2], (GROUP_SIZE, GROUP_SIZE), 0, hot_rows)
    cold_off = jax.random.randint(route_keys[3], (GROUP_SIZE, GROUP_SIZE), 0, cold_rows)
    hot_pick = (jnp.take_along_axis(hot_off, src_of, axis=1) + within) % hot_rows
    cold_pick = hot_rows + (jnp.take_along_axis(cold_off, src_of, axis=1) + within - hot_count) % cold_rows
    local_rank = jnp.where(within < hot_count, hot_pick, cold_pick)
    row_grid = jnp.tile(jnp.arange(tok_local, dtype=jnp.int32)[None, :], (GROUP_SIZE, 1))
    row_order = jax.random.permutation(route_keys[4], row_grid, axis=1, independent=True).reshape(-1)
    chosen = src_of * tok_local + row_order[src_of * tok_local + local_rank]
    chosen = chosen.reshape(EXPERTS, CAPACITY)
    return jax.random.permutation(route_keys[5], chosen, axis=1, independent=True)


def setup_inputs(seed: int = 0, part: int = 0) -> dict:
    base_key = jax.random.key(seed)
    shared_keys = jax.random.split(base_key, 2)
    part_keys = jax.random.split(jax.random.fold_in(base_key, part), 3)
    tokens = jax.random.normal(part_keys[0], (TOKENS, D_MODEL), jnp.float32).astype(jnp.bfloat16)
    choice_idx = draw_routing(part_keys[1])
    gate_weight = jax.random.uniform(part_keys[2], (EXPERTS, CAPACITY), jnp.float32, 0.5, 1.5)
    w_in = (jax.random.normal(shared_keys[0], (EXPERTS, D_MODEL, D_FF), jnp.float32) * D_MODEL ** -0.5).astype(jnp.bfloat16)
    w_out = (jax.random.normal(shared_keys[1], (EXPERTS, D_FF, D_MODEL), jnp.float32) * D_FF ** -0.5).astype(jnp.bfloat16)
    return {"tokens": tokens, "choice_idx": choice_idx, "gate_weight": gate_weight, "w_in": w_in, "w_out": w_out}


def reference(tokens, choice_idx, gate_weight, w_in, w_out):
    def expert_step(acc_sum, per_expert):
        idx_row, gate_row, w_first, w_second = per_expert
        tok_rows = tokens[idx_row]
        pre_act = jnp.dot(tok_rows, w_first, preferred_element_type=jnp.float32)
        hidden = jax.nn.gelu(pre_act, approximate=True).astype(jnp.bfloat16)
        expert_out = jnp.dot(hidden, w_second, preferred_element_type=jnp.float32)
        weighted = (gate_row[:, None] * expert_out).astype(jnp.bfloat16)
        return acc_sum.at[idx_row].add(weighted.astype(jnp.float32)), None

    zero_acc = jnp.zeros((TOKENS, D_MODEL), jnp.float32)
    acc_sum = lax.scan(expert_step, zero_acc, (choice_idx, gate_weight, w_in, w_out))[0]
    return (tokens.astype(jnp.float32) + acc_sum).astype(jnp.bfloat16)
```

```python
import jax
import jax.numpy as jnp
from jax import lax
from jax.experimental import pallas as pl
from jax.experimental.pallas import tpu as pltpu
from jax.sharding import PartitionSpec as P


def _windows(starts, sel, gate, group_n, width):
    tall = width // 128

    def body(st_ref, sel_ref, gate_ref, osel_ref, ogate_ref):
        def step(s, carry):
            st = st_ref[s]
            row = st // 128
            off = st % 128
            lane = lax.broadcasted_iota(jnp.int32, (8, 128), 1)
            for src, dst in ((sel_ref, osel_ref), (gate_ref, ogate_ref)):
                blk = src[pl.ds(row, 8), :]
                y = pltpu.roll(blk, lax.rem(128 - off, 128), 1)
                z = pltpu.roll(y, 7, 0)
                dst[s] = jnp.where(lane < 128 - off, y, z)[:tall]
            return carry

        lax.fori_loop(0, group_n, step, 0)

    n = sel.shape[0]
    pad = 8 * 128
    sel2 = jnp.pad(sel, (0, pad)).reshape(-1, 128)
    gate2 = jnp.pad(gate, (0, pad)).reshape(-1, 128)
    return pl.pallas_call(
        body,
        grid_spec=pltpu.PrefetchScalarGridSpec(
            num_scalar_prefetch=1,
            grid=(),
            in_specs=[pl.BlockSpec(memory_space=pltpu.VMEM)] * 2,
            out_specs=[pl.BlockSpec(memory_space=pltpu.VMEM)] * 2,
        ),
        out_shape=[
            jax.ShapeDtypeStruct((group_n, tall, 128), jnp.int32),
            jax.ShapeDtypeStruct((group_n, tall, 128), jnp.float32),
        ],
    )(starts, sel2, gate2)


def solution(mesh):
    group_n = mesh.shape["ep"]
    row_spec = P(("dp", "ep"), None)
    expert_spec = P("ep", None, None)

    def local_layer(tok_loc, sel_loc, gate_loc, win_loc, wout_loc):
        tok_count, model_dim = tok_loc.shape
        exp_count, cap_slots = sel_loc.shape
        n = exp_count * cap_slots
        pair_cap = 2 * n // group_n
        sel, gate = lax.sort((sel_loc.reshape(n), gate_loc.reshape(n)), num_keys=1)
        bounds = jnp.arange(group_n + 1, dtype=jnp.int32) * tok_count
        edges = jnp.sum((sel[None, :] < bounds[:, None]).astype(jnp.int32), axis=1)
        counts = edges[1:] - edges[:-1]
        wsel, wgate = _windows(edges[:-1], sel, gate, group_n, pair_cap)
        lane = jnp.arange(pair_cap, dtype=jnp.int32)
        request = jnp.where(lane[None] < counts[:, None], wsel.reshape(group_n, pair_cap) - bounds[:-1, None], -1)
        wgate = wgate.reshape(group_n, pair_cap)
        asked = lax.all_to_all(request, "ep", 0, 0, tiled=True)
        cuts = (0, pair_cap // 8, pair_cap * 9 // 16, pair_cap)
        parts = [slice(cuts[i], cuts[i + 1]) for i in range(3)]
        got = []
        for part in parts:
            idx = jnp.maximum(asked[:, part], 0).reshape(-1)
            rows = tok_loc[idx].reshape(group_n, part.stop - part.start, model_dim)
            got.append(lax.all_to_all(rows, "ep", 0, 0, tiled=True))
        weighted = []
        for part, x in zip(parts, got):
            pre = jnp.dot(x.reshape(-1, model_dim), win_loc[0], preferred_element_type=jnp.float32)
            hidden = jax.nn.gelu(pre, approximate=True).astype(jnp.bfloat16)
            o = jnp.dot(hidden, wout_loc[0], preferred_element_type=jnp.float32)
            g = wgate[:, part].reshape(-1)
            weighted.append((g[:, None] * o).astype(jnp.bfloat16).reshape(x.shape))

        def add_rows(acc, part, rows):
            idx = asked[:, part].reshape(-1)
            at = jnp.where(idx < 0, tok_count, idx)
            return acc.at[at].add(rows.reshape(-1, model_dim).astype(jnp.float32), mode="drop")

        acc = tok_loc.astype(jnp.float32)
        back1 = lax.all_to_all(weighted[1], "ep", 0, 0, tiled=True)
        back2 = lax.all_to_all(weighted[2], "ep", 0, 0, tiled=True)
        acc = add_rows(acc, parts[1], back1)
        last, acc, back2 = lax.optimization_barrier((weighted[0], acc, back2))
        back0 = lax.all_to_all(last, "ep", 0, 0, tiled=True)
        acc = add_rows(acc, parts[2], back2)
        acc = add_rows(acc, parts[0], back0)
        return acc.astype(jnp.bfloat16)

    return jax.shard_map(local_layer, mesh=mesh, in_specs=(row_spec, row_spec, row_spec, expert_spec, expert_spec), out_specs=row_spec, check_vma=False)
```

```python
import jax
import jax.numpy as jnp
from jax import lax
from jax.experimental import pallas as pl
from jax.experimental.pallas import tpu as pltpu
from jax.sharding import PartitionSpec as P


def _windows(starts, sel, gate, group_n, width):
    tall = width // 128

    def body(st_ref, sel_ref, gate_ref, osel_ref, ogate_ref):
        def step(s, carry):
            st = st_ref[s]
            row = st // 128
            off = st % 128
            lane = lax.broadcasted_iota(jnp.int32, (8, 128), 1)
            for src, dst in ((sel_ref, osel_ref), (gate_ref, ogate_ref)):
                blk = src[pl.ds(row, 8), :]
                y = pltpu.roll(blk, lax.rem(128 - off, 128), 1)
                z = pltpu.roll(y, 7, 0)
                dst[s] = jnp.where(lane < 128 - off, y, z)[:tall]
            return carry

        lax.fori_loop(0, group_n, step, 0)

    n = sel.shape[0]
    pad = 8 * 128
    sel2 = jnp.pad(sel, (0, pad)).reshape(-1, 128)
    gate2 = jnp.pad(gate, (0, pad)).reshape(-1, 128)
    return pl.pallas_call(
        body,
        grid_spec=pltpu.PrefetchScalarGridSpec(
            num_scalar_prefetch=1,
            grid=(),
            in_specs=[pl.BlockSpec(memory_space=pltpu.VMEM)] * 2,
            out_specs=[pl.BlockSpec(memory_space=pltpu.VMEM)] * 2,
        ),
        out_shape=[
            jax.ShapeDtypeStruct((group_n, tall, 128), jnp.int32),
            jax.ShapeDtypeStruct((group_n, tall, 128), jnp.float32),
        ],
    )(starts, sel2, gate2)


def solution(mesh):
    group_n = mesh.shape["ep"]
    row_spec = P(("dp", "ep"), None)
    expert_spec = P("ep", None, None)

    def local_layer(tok_loc, sel_loc, gate_loc, win_loc, wout_loc):
        tok_count, model_dim = tok_loc.shape
        exp_count, cap_slots = sel_loc.shape
        n = exp_count * cap_slots
        pair_cap = 2 * n // group_n
        sel, gate = lax.sort((sel_loc.reshape(n), gate_loc.reshape(n)), num_keys=1)
        bounds = jnp.arange(group_n + 1, dtype=jnp.int32) * tok_count
        edges = jnp.sum((sel[None, :] < bounds[:, None]).astype(jnp.int32), axis=1)
        counts = edges[1:] - edges[:-1]
        wsel, wgate = _windows(edges[:-1], sel, gate, group_n, pair_cap)
        lane = jnp.arange(pair_cap, dtype=jnp.int32)
        request = jnp.where(lane[None] < counts[:, None], wsel.reshape(group_n, pair_cap) - bounds[:-1, None], -1)
        wgate = wgate.reshape(group_n, pair_cap)
        asked = lax.all_to_all(request, "ep", 0, 0, tiled=True)
        cuts = (0, pair_cap // 16, pair_cap * 3 // 16, pair_cap * 19 // 32, pair_cap)
        parts = [slice(cuts[i], cuts[i + 1]) for i in range(4)]
        got = []
        for part in parts:
            idx = jnp.maximum(asked[:, part], 0).reshape(-1)
            rows = tok_loc[idx].reshape(group_n, part.stop - part.start, model_dim)
            if got:
                rows, got[-1] = lax.optimization_barrier((rows, got[-1]))
            got.append(lax.all_to_all(rows, "ep", 0, 0, tiled=True))
        weighted = []
        for part, x in zip(parts, got):
            pre = jnp.dot(x.reshape(-1, model_dim), win_loc[0], preferred_element_type=jnp.float32)
            hidden = jax.nn.gelu(pre, approximate=True).astype(jnp.bfloat16)
            o = jnp.dot(hidden, wout_loc[0], preferred_element_type=jnp.float32)
            g = wgate[:, part].reshape(-1)
            weighted.append((g[:, None] * o).astype(jnp.bfloat16).reshape(x.shape))

        def add_rows(acc, part, rows):
            idx = asked[:, part].reshape(-1)
            at = jnp.where(idx < 0, tok_count, idx)
            return acc.at[at].add(rows.reshape(-1, model_dim).astype(jnp.float32), mode="drop")

        acc = tok_loc.astype(jnp.float32)
        back2 = lax.all_to_all(weighted[2], "ep", 0, 0, tiled=True)
        back3 = lax.all_to_all(weighted[3], "ep", 0, 0, tiled=True)
        acc = add_rows(acc, parts[2], back2)
        short, weighted[0], acc, back3 = lax.optimization_barrier((weighted[1], weighted[0], acc, back3))
        back1 = lax.all_to_all(short, "ep", 0, 0, tiled=True)
        acc = add_rows(acc, parts[3], back3)
        short, acc, back1 = lax.optimization_barrier((weighted[0], acc, back1))
        back0 = lax.all_to_all(short, "ep", 0, 0, tiled=True)
        acc = add_rows(acc, parts[1], back1)
        acc = add_rows(acc, parts[0], back0)
        return acc.astype(jnp.bfloat16)

    return jax.shard_map(local_layer, mesh=mesh, in_specs=(row_spec, row_spec, row_spec, expert_spec, expert_spec), out_specs=row_spec, check_vma=False)
```

```python
import jax
import jax.numpy as jnp
from jax import lax
from jax.experimental import pallas as pl
from jax.experimental.pallas import tpu as pltpu
from jax.sharding import PartitionSpec as P


def _windows(starts, sel, gate, group_n, width):
    tall = width // 128

    def body(st_ref, sel_ref, gate_ref, osel_ref, ogate_ref):
        def step(s, carry):
            st = st_ref[s]
            row = st // 128
            off = st % 128
            lane = lax.broadcasted_iota(jnp.int32, (8, 128), 1)
            for src, dst in ((sel_ref, osel_ref), (gate_ref, ogate_ref)):
                blk = src[pl.ds(row, 8), :]
                y = pltpu.roll(blk, lax.rem(128 - off, 128), 1)
                z = pltpu.roll(y, 7, 0)
                dst[s] = jnp.where(lane < 128 - off, y, z)[:tall]
            return carry

        lax.fori_loop(0, group_n, step, 0)

    n = sel.shape[0]
    pad = 8 * 128
    sel2 = jnp.pad(sel, (0, pad)).reshape(-1, 128)
    gate2 = jnp.pad(gate, (0, pad)).reshape(-1, 128)
    return pl.pallas_call(
        body,
        grid_spec=pltpu.PrefetchScalarGridSpec(
            num_scalar_prefetch=1,
            grid=(),
            in_specs=[pl.BlockSpec(memory_space=pltpu.VMEM)] * 2,
            out_specs=[pl.BlockSpec(memory_space=pltpu.VMEM)] * 2,
        ),
        out_shape=[
            jax.ShapeDtypeStruct((group_n, tall, 128), jnp.int32),
            jax.ShapeDtypeStruct((group_n, tall, 128), jnp.float32),
        ],
    )(starts, sel2, gate2)


def solution(mesh):
    group_n = mesh.shape["ep"]
    row_spec = P(("dp", "ep"), None)
    expert_spec = P("ep", None, None)

    def local_layer(tok_loc, sel_loc, gate_loc, win_loc, wout_loc):
        tok_count, model_dim = tok_loc.shape
        exp_count, cap_slots = sel_loc.shape
        n = exp_count * cap_slots
        pair_cap = 2 * n // group_n
        sel, gate = lax.sort((sel_loc.reshape(n), gate_loc.reshape(n)), num_keys=1)
        bounds = jnp.arange(group_n + 1, dtype=jnp.int32) * tok_count
        edges = jnp.sum((sel[None, :] < bounds[:, None]).astype(jnp.int32), axis=1)
        counts = edges[1:] - edges[:-1]
        wsel, wgate = _windows(edges[:-1], sel, gate, group_n, pair_cap)
        lane = jnp.arange(pair_cap, dtype=jnp.int32)
        request = jnp.where(lane[None] < counts[:, None], wsel.reshape(group_n, pair_cap) - bounds[:-1, None], -1)
        wgate = wgate.reshape(group_n, pair_cap)
        asked = lax.all_to_all(request, "ep", 0, 0, tiled=True)
        cuts = (0, pair_cap * 5 // 32, pair_cap * 37 // 64, pair_cap)
        parts = [slice(cuts[i], cuts[i + 1]) for i in range(3)]
        got = []
        for part in parts:
            idx = jnp.maximum(asked[:, part], 0).reshape(-1)
            rows = tok_loc[idx].reshape(group_n, part.stop - part.start, model_dim)
            got.append(lax.all_to_all(rows, "ep", 0, 0, tiled=True))
        weighted = []
        for part, x in zip(parts, got):
            pre = jnp.dot(x.reshape(-1, model_dim), win_loc[0], preferred_element_type=jnp.float32)
            hidden = jax.nn.gelu(pre, approximate=True).astype(jnp.bfloat16)
            o = jnp.dot(hidden, wout_loc[0], preferred_element_type=jnp.float32)
            g = wgate[:, part].reshape(-1)
            weighted.append((g[:, None] * o).astype(jnp.bfloat16).reshape(x.shape))

        def add_rows(acc, part, rows):
            idx = asked[:, part].reshape(-1)
            at = jnp.where(idx < 0, tok_count, idx)
            return acc.at[at].add(rows.reshape(-1, model_dim).astype(jnp.float32), mode="drop")

        acc = tok_loc.astype(jnp.float32)
        back1 = lax.all_to_all(weighted[1], "ep", 0, 0, tiled=True)
        back2 = lax.all_to_all(weighted[2], "ep", 0, 0, tiled=True)
        acc = add_rows(acc, parts[1], back1)
        last, acc, back2 = lax.optimization_barrier((weighted[0], acc, back2))
        back0 = lax.all_to_all(last, "ep", 0, 0, tiled=True)
        acc = add_rows(acc, parts[2], back2)
        acc = add_rows(acc, parts[0], back0)
        return acc.astype(jnp.bfloat16)

    return jax.shard_map(local_layer, mesh=mesh, in_specs=(row_spec, row_spec, row_spec, expert_spec, expert_spec), out_specs=row_spec, check_vma=False)
```
